32 devices in a mesh: groups: 2 (over x), dp: 16 (over z, y, core).
Axes of the slice: x: 2, y: 2, z: 4, core: 2. Of those that a mesh axis runs over, the one named last changes fastest.
Arguments:
- queries: bfloat16 [24576, 4096], P(('groups', 'dp')), parts along dimension 0, may hold values from -120 to 120
- keys: bfloat16 [24576, 512], P(('groups', 'dp')), parts along dimension 0, may hold values from -6 to 6
- values: bfloat16 [24576, 512], P(('groups', 'dp')), parts along dimension 0, may hold values from -6 to 6
- block_counts: int32 [32], P(('groups', 'dp')), parts along dimension 0, may hold values from 0 to 6, as said below
- segment_ids: int32 [8192], P(('groups', 'dp')), parts along dimension 0, may hold values from 0 to 7, never falling along the last dimension, each value on 1 to 1024 neighbouring positions
- reward_dir: float32 [4096], replicated, may hold values from -4 to 4
Outputs:
- attn_out: bfloat16 [8192, 4096], P(('groups', 'dp')), parts along dimension 0
- rewards: float32 [16], P('groups'), parts along dimension 0
The draws below stay inside these ranges and needn't reach their ends.
There are 2 independent parts, one for each index of `groups`. The reference program is written for one: setup_inputs(seed, part) draws one part's arguments, and reference() takes and returns one part's arrays. A program takes and returns all parts, laid end to end along the dimension named above; an argument that names none is the same for every part. Nothing has to cross between parts.
Inputs may be any that keep to these rules, and one draw needn't show every extreme that they name: `block_counts`: the counts sum to 2 times the number of ranks; for each rank s the counts of the ranks before s sum to between (2 * s - 2) and (2 * s + 2); some rank holds 6. `segment_ids`: positions never fall in segment number, each of the 8 responses holds 1 to 1024 positions.
All inputs are finite; a program needn't handle non-finite values.
Results may differ from the reference program's by a relative error of at most 0.0039.
The reference program's roundings to bfloat16 on the way (of `soft_weights`) count: a program that leaves them out, or rounds other values in their place, can miss the bound.
Values may be sent and summed in bfloat16 or wider, within the bound.
No kernel may reach another device: no remote copies, remote signals or barrier semaphores. Data moves between devices by JAX's collectives and lax.ppermute only.
A program may use at most 128 MiB of HBM per device.

```python
import math
import jax
import jax.numpy as jnp
import numpy as np
from jax import lax

D_HEAD = 128
HEADS = 32
KV_HEADS = 4
BLOCK = 128
RECV = 2
REACH = 4
CAP = 6
TOKENS = 4096
SRC_TOK = 12288
MAXLEN = 1024
NRESP = 8
N_DP = 16


def pair_draw(key):
    query_key = jax.random.fold_in(key, 11)
    key_key = jax.random.fold_in(key, 12)
    key_rows = jnp.clip(jax.random.normal(key_key, (SRC_TOK, KV_HEADS * D_HEAD), jnp.float32), -6.0, 6.0)
    query_rows = jnp.clip(jax.random.normal(query_key, (SRC_TOK, HEADS * D_HEAD), jnp.float32), -6.0, 6.0)
    return (query_rows, key_rows)


def draw_queries(key, part):
    return pair_draw(key)[0].astype(jnp.bfloat16)


def draw_keys(key, part):
    return pair_draw(key)[1].astype(jnp.bfloat16)


def draw_block_counts(key, part):
    marker = jnp.arange(N_DP + 1, dtype=jnp.int32)
    peak_rank = jax.random.randint(jax.random.fold_in(key, 22), (), 2, N_DP - 2).astype(jnp.int32)
    peak_rank = jnp.where(peak_rank >= N_DP // 2, peak_rank + 1, peak_rank).astype(jnp.int32)
    turn_rank = jax.random.randint(jax.random.fold_in(key, 23), (), 0, peak_rank - 1).astype(jnp.int32)
    excess = jnp.zeros((N_DP + 1,), jnp.int32)
    excess = jnp.where((marker >= 1) & (marker <= turn_rank), RECV, excess)
    excess = jnp.where((marker >= turn_rank + 2) & (marker <= peak_rank), -RECV, excess)
    excess = jnp.where((marker >= peak_rank + 1) & (marker <= N_DP - 1), RECV, excess)
    return (RECV + excess[1:] - excess[:-1]).astype(jnp.int32)


def block_levels(own_key, dims, cuts, least, high):
    factor_of = 1.0
    for position, parts in cuts:
        draws = jax.random.uniform(jax.random.fold_in(jax.random.fold_in(own_key, 6), position), (parts,), jnp.float32, least / len(cuts), high / len(cuts))
        factor_of = factor_of * jnp.repeat(jnp.exp(draws), dims[position] // parts).reshape((-1,) + (1,) * (len(dims) - 1 - position))
    return factor_of


def profile(amount, total, most, lean):
    loads = [(1 << 20) // math.isqrt(standing ** lean) + 1 for standing in range(2, amount + 1)]
    surplus, given = total - most - (amount - 1), [1] * (amount - 1)
    while surplus > 0:
        movable = [i for i in range(amount - 1) if given[i] < most]
        mass, budget = sum([loads[i] for i in movable]), surplus
        for i in movable:
            addition = min(most - given[i], max(1, budget * loads[i] // mass), surplus)
            given[i] = given[i] + addition
            surplus = surplus - addition
    return np.array([most] + given)


def ragged_sizes(own_key, number_of, total, most, skew):
    if number_of == 2:
        one = jax.random.randint(own_key, (), max(1, total - most), min(most, total - 1) + 1)
        return jnp.stack([one, total - one])
    sizes = jnp.asarray(profile(number_of, total, most, skew), jnp.int32)
    twos = (number_of - 1) // 2
    giver, taker = sizes[1:1 + 2 * twos:2], sizes[2:2 + 2 * twos:2]
    margin = jnp.minimum(giver - 1, most - taker)
    passed = jax.random.randint(jax.random.fold_in(own_key, 1), (twos,), 0, 1 << 20) % (margin + 1)
    sizes = sizes.at[1:1 + 2 * twos:2].set(giver - passed).at[2:2 + 2 * twos:2].set(taker + passed)
    return sizes[jax.random.permutation(jax.random.fold_in(own_key, 2), number_of)]


def bell_draw(rng, extent, spread, most, shards=(), held_as=jnp.bfloat16):
    result = spread * jax.random.normal(rng, extent, jnp.float32)
    if shards:
        result = result * block_levels(rng, extent, shards, -0.22, 0.18)
    return jnp.clip(result, -most, most).astype(held_as)


def setup_inputs(seed: int = 0, part: int = 0) -> dict:
    key_of = jax.random.split(jax.random.key(seed), 7)
    part_splits = jax.random.split(jax.random.fold_in(key_of[6], part), 7)
    queries = draw_queries(jax.random.fold_in(jax.random.fold_in(key_of[6], part), 71), part)
    keys = draw_keys(jax.random.fold_in(jax.random.fold_in(key_of[6], part), 71), part)
    values = bell_draw(part_splits[2], (SRC_TOK, KV_HEADS * D_HEAD), 1.0, 6.0, ((0, 16),))
    block_counts = draw_block_counts(jax.random.fold_in(jax.random.fold_in(key_of[6], part), 71), part)
    segment_ids = jnp.searchsorted(jnp.cumsum(ragged_sizes(part_splits[4], NRESP, TOKENS, MAXLEN, 1)), jnp.arange(TOKENS), side="right").astype(jnp.int32)
    reward_dir = bell_draw(key_of[5], (HEADS * D_HEAD,), 0.25, 4.0, (), jnp.float32)
    return {"queries": queries, "keys": keys, "values": values, "block_counts": block_counts, "segment_ids": segment_ids, "reward_dir": reward_dir}


def attend(query_rows, key_window, value_window, allowed):
    per_group = HEADS // KV_HEADS
    row_count = query_rows.shape[0]
    score_scale = D_HEAD ** -0.5
    grouped = query_rows.reshape(row_count, KV_HEADS, per_group, D_HEAD)
    key_heads = key_window.reshape(-1, KV_HEADS, D_HEAD)
    value_heads = value_window.reshape(-1, KV_HEADS, D_HEAD)
    head_outs = []
    for head_index in range(KV_HEADS):
        query_head = grouped[:, head_index].reshape(row_count * per_group, D_HEAD)
        logits = jnp.dot(query_head, key_heads[:, head_index].T, preferred_element_type=jnp.float32) * score_scale
        logits = logits.reshape(row_count, per_group, -1)
        logits = jnp.where(allowed[:, None, :], logits, -1e30)
        row_max = jnp.max(logits, axis=-1, keepdims=True)
        raised = jnp.exp(logits - row_max)
        totals = jnp.sum(raised, axis=-1)
        soft_weights = raised.astype(jnp.bfloat16).reshape(row_count * per_group, -1)
        head_out = jnp.dot(soft_weights, value_heads[:, head_index], preferred_element_type=jnp.float32)
        head_out = head_out.reshape(row_count, per_group, D_HEAD) / totals[..., None]
        head_outs.append(head_out.astype(jnp.bfloat16))
    return jnp.stack(head_outs, axis=1).reshape(row_count, HEADS * D_HEAD)


def reference(queries, keys, values, block_counts, segment_ids, reward_dir):
    row_count = RECV * BLOCK
    offsets = (jnp.cumsum(block_counts) - block_counts).astype(jnp.int32)
    slot_index = jnp.arange(CAP, dtype=jnp.int32)
    target = offsets[:, None] + slot_index[None, :]
    target = jnp.where(slot_index[None, :] < block_counts[:, None], target, N_DP * RECV).reshape(-1)

    def arrange(source):
        blocks = source.reshape(N_DP * CAP, BLOCK, source.shape[1])
        placed = jnp.zeros((N_DP * RECV, BLOCK, source.shape[1]), source.dtype)
        placed = placed.at[target].set(blocks, mode="drop")
        return placed.reshape(N_DP * RECV * BLOCK, source.shape[1])

    packed_queries = arrange(queries)
    packed_keys = arrange(keys)
    packed_values = arrange(values)
    positions = jnp.arange(TOKENS, dtype=jnp.int32)
    changed = jnp.concatenate([jnp.ones((1,), bool), segment_ids[1:] != segment_ids[:-1]])
    starts = lax.cummax(jnp.where(changed, positions, 0).astype(jnp.int32), axis=0)
    is_last = jnp.concatenate([segment_ids[1:] != segment_ids[:-1], jnp.ones((1,), bool)])
    reach_rows = REACH * row_count
    padded_keys = jnp.concatenate([jnp.zeros((reach_rows, packed_keys.shape[1]), jnp.bfloat16), packed_keys])
    padded_values = jnp.concatenate([jnp.zeros((reach_rows, packed_values.shape[1]), jnp.bfloat16), packed_values])

    def one_block(block_index):
        row_start = (block_index * row_count).astype(jnp.int32)
        query_rows = lax.dynamic_slice_in_dim(packed_queries, row_start, row_count, 0)
        key_window = lax.dynamic_slice_in_dim(padded_keys, row_start, reach_rows + row_count, 0)
        value_window = lax.dynamic_slice_in_dim(padded_values, row_start, reach_rows + row_count, 0)
        key_pos = row_start - reach_rows + jnp.arange(reach_rows + row_count, dtype=jnp.int32)
        query_pos = row_start + jnp.arange(row_count, dtype=jnp.int32)
        query_starts = lax.dynamic_slice_in_dim(starts, row_start, row_count, 0)
        allowed = (key_pos[None, :] >= query_starts[:, None]) & (key_pos[None, :] <= query_pos[:, None])
        return attend(query_rows, key_window, value_window, allowed)

    attn_out = lax.map(one_block, jnp.arange(N_DP, dtype=jnp.int32)).reshape(TOKENS, HEADS * D_HEAD)
    token_score = jnp.dot(attn_out.astype(jnp.float32), reward_dir, precision=lax.Precision.HIGHEST)
    rewards = jnp.zeros((NRESP,), jnp.float32).at[segment_ids].add(jnp.where(is_last, token_score, 0.0))
    return attn_out, rewards
```

```python
import functools
import math

import jax
import jax.numpy as jnp
from jax import lax
from jax.experimental import pallas as pl
from jax.experimental.pallas import tpu as pltpu
from jax.sharding import PartitionSpec as P

D_HEAD = 128
HEADS = 32
KV_HEADS = 4
BLOCK = 128
RECV = 2
REACH = 4
PER_GROUP = HEADS // KV_HEADS
ROWS = RECV * BLOCK
PIECES = REACH + 1
KV_WIDTH = KV_HEADS * D_HEAD
CHUNK = PER_GROUP * D_HEAD
MASKED = -1e30
EXP2_SCALE = D_HEAD ** (-0.5) * math.log2(math.e)


def shifted(block, axis, distance):
    devices = range(lax.axis_size(axis))
    route = [(i - distance, i) for i in devices if i - distance in devices]
    return lax.ppermute(block, axis, route)


def placement(info, place, responses, ranks):
    rank = place[0]
    before = lax.fori_loop(
        0, ranks, lambda s, t: t + jnp.where(s < rank, info[responses + s], 0), jnp.int32(0)
    )
    left_count = info[responses + jnp.maximum(rank - 1, 0)]
    return rank, before - rank * RECV, info[responses + rank], left_count


def pick(k, excess, count, left_count, capacity):
    left_first = jnp.clip(left_count - RECV, 0, capacity - RECV)
    from_left = k < excess
    slot = k - excess
    is_own = jnp.logical_and(jnp.logical_not(from_left), slot < count)
    kind = jnp.where(from_left, 0, jnp.where(is_own, 1, 2))
    index = jnp.where(
        from_left, left_count - excess + k - left_first, jnp.where(is_own, slot, slot - count)
    )
    limit = jnp.where(is_own, capacity - 1, RECV - 1)
    return kind, jnp.clip(index, 0, limit)


def block_rows(index):
    return pl.ds(pl.multiple_of(index * BLOCK, BLOCK), BLOCK)


def pack_kernel(responses, ranks, capacity, info, place, keys, values, left, right, out, sems):
    _, excess, count, left_count = placement(info, place, responses, ranks)
    jobs = []
    for k in range(RECV):
        kind, index = pick(k, excess, count, left_count, capacity)
        rows = block_rows(index)
        into = pl.ds(k * BLOCK, BLOCK)
        key_part, value_part = pl.ds(0, KV_WIDTH), pl.ds(KV_WIDTH, KV_WIDTH)
        own_keys = pltpu.make_async_copy(keys.at[rows], out.at[into, key_part], sems.at[k, 0])
        own_values = pltpu.make_async_copy(values.at[rows], out.at[into, value_part], sems.at[k, 1])
        from_left = pltpu.make_async_copy(left.at[rows], out.at[into], sems.at[k, 2])
        from_right = pltpu.make_async_copy(right.at[rows], out.at[into], sems.at[k, 3])
        jobs.append((kind, ((0, from_left), (1, own_keys), (1, own_values), (2, from_right))))
    for kind, copies in jobs:
        for wanted, copy in copies:
            pl.when(kind == wanted)(copy.start)
    for kind, copies in jobs:
        for wanted, copy in copies:
            pl.when(kind == wanted)(copy.wait)


def pack(info, place, keys, values, left, right, responses, ranks):
    capacity = keys.shape[0] // BLOCK
    smem = pl.BlockSpec(memory_space=pltpu.SMEM)
    anywhere = pl.BlockSpec(memory_space=pl.ANY)
    return pl.pallas_call(
        functools.partial(pack_kernel, responses, ranks, capacity),
        out_shape=jax.ShapeDtypeStruct((ROWS, 2 * KV_WIDTH), keys.dtype),
        in_specs=[smem, smem] + [anywhere] * 4,
        out_specs=pl.BlockSpec(memory_space=pltpu.VMEM),
        scratch_shapes=[pltpu.SemaphoreType.DMA((RECV, 4))],
        name="pack",
    )(info, place, keys, values, left, right)


def attend_kernel(
    responses, ranks, capacity, chunk,
    info, place, queries, q_left, q_right, own, two, four, sib_own, sib_two, sib_four, reward_dir,
    out, score, kbuf, vbuf, qbuf, obuf, sbuf, mbuf, lbuf, abuf, q_sems, kv_sems, o_sems,
):
    rank, excess, count, left_count = placement(info, place, responses, ranks)
    odd = lax.rem(rank, 2) == 1
    columns = pl.ds(chunk * CHUNK, CHUNK)

    q_jobs = []
    for k in range(RECV):
        kind, index = pick(k, excess, count, left_count, capacity)
        rows = block_rows(index)
        q_jobs.append((kind, (
            pltpu.make_async_copy(q_left.at[rows], qbuf.at[k], q_sems.at[k, 0]),
            pltpu.make_async_copy(queries.at[rows, columns], qbuf.at[k], q_sems.at[k, 1]),
            pltpu.make_async_copy(q_right.at[rows], qbuf.at[k], q_sems.at[k, 2]),
        )))

    def piece_copies(source, piece):
        return [
            pltpu.make_async_copy(
                source.at[:, pl.ds(chunk * D_HEAD, D_HEAD)], kbuf.at[piece], kv_sems.at[piece, 0]
            ),
            pltpu.make_async_copy(
                source.at[:, pl.ds(KV_WIDTH + chunk * D_HEAD, D_HEAD)],
                vbuf.at[piece], kv_sems.at[piece, 1],
            ),
        ]

    even = jnp.logical_not(odd)
    kv_jobs = [(None, piece_copies(own, 4)), (None, piece_copies(two, 2)), (None, piece_copies(four, 0))]
    kv_jobs += [(even, piece_copies(sib_two, 3)), (odd, piece_copies(sib_own, 3))]
    kv_jobs += [(even, piece_copies(sib_four, 1)), (odd, piece_copies(sib_two, 1))]

    def each(action):
        for kind, copies in q_jobs:
            for wanted, copy in enumerate(copies):
                pl.when(kind == wanted)(getattr(copy, action))
        for condition, copies in kv_jobs:
            for copy in copies:
                if condition is None:
                    getattr(copy, action)()
                else:
                    pl.when(condition)(getattr(copy, action))

    each("start")

    window_base = (rank - REACH) * ROWS
    row_iota = lax.broadcasted_iota(jnp.int32, (BLOCK, D_HEAD), 0)
    lane_iota = lax.broadcasted_iota(jnp.int32, (BLOCK, D_HEAD), 1)
    plan = []
    for k in range(RECV):
        first = rank * ROWS + k * BLOCK
        rows_at = row_iota + first

        def widen(r, carry):
            begin, begins = carry
            start = info[r]
            begin = jnp.where(start <= first, jnp.maximum(begin, start), begin)
            begins = jnp.where(rows_at >= start, jnp.maximum(begins, start), begins)
            return begin, begins

        begin, begins = lax.fori_loop(
            0, responses, widen, (jnp.int32(0), jnp.zeros((BLOCK, D_HEAD), jnp.int32))
        )
        lowest = jnp.clip((begin - window_base) // ROWS, 0, REACH)
        plan.append((lowest, begins, rows_at))

    each("wait")

    pair = 2
    for k in range(RECV):
        lowest, begins, rows_at = plan[k]
        mbuf[...] = jnp.full_like(mbuf, MASKED)

        def score_tile(p, _):
            base = window_base + p * ROWS
            masks = []
            for half in range(2):
                at = lane_iota + (base + half * D_HEAD)
                masks.append(jnp.logical_and(at >= begins, at <= rows_at))
            key_tile = kbuf[p]
            for j in range(0, PER_GROUP, pair):
                heads = [qbuf[k, :, (j + i) * D_HEAD:(j + i + 1) * D_HEAD] for i in range(pair)]
                logits = lax.dot_general(
                    jnp.concatenate(heads, axis=0), key_tile, (((1,), (1,)), ((), ())),
                    preferred_element_type=jnp.float32,
                )
                for i in range(pair):
                    rows = pl.ds((j + i) * BLOCK, BLOCK)
                    part = logits[i * BLOCK:(i + 1) * BLOCK]
                    low = jnp.where(masks[0], part[:, :D_HEAD], MASKED)
                    high = jnp.where(masks[1], part[:, D_HEAD:], MASKED)
                    sbuf[p, rows, :D_HEAD] = low
                    sbuf[p, rows, D_HEAD:] = high
                    mbuf[rows, :] = jnp.maximum(mbuf[rows, :], jnp.maximum(low, high))
            return 0

        lax.fori_loop(lowest, PIECES, score_tile, 0)
        for j in range(PER_GROUP):
            rows = pl.ds(j * BLOCK, BLOCK)
            peak = jnp.max(mbuf[rows, :], axis=-1, keepdims=True)
            mbuf[rows, :] = jnp.broadcast_to(peak, (BLOCK, D_HEAD))
        lbuf[...] = jnp.zeros_like(lbuf)
        abuf[...] = jnp.zeros_like(abuf)

        def weigh_tile(p, _):
            value_tile = vbuf[p]
            for j in range(0, PER_GROUP, pair):
                rows = pl.ds(j * BLOCK, pair * BLOCK)
                peak = mbuf[rows, :]
                low = jnp.exp2((sbuf[p, rows, :D_HEAD] - peak) * EXP2_SCALE)
                high = jnp.exp2((sbuf[p, rows, D_HEAD:] - peak) * EXP2_SCALE)
                lbuf[rows, :] += low + high
                soft = jnp.concatenate([low.astype(jnp.bfloat16), high.astype(jnp.bfloat16)], axis=1)
                abuf[rows, :] += jnp.dot(soft, value_tile, preferred_element_type=jnp.float32)
            return 0

        lax.fori_loop(lowest, PIECES, weigh_tile, 0)
        scored = jnp.zeros((BLOCK, D_HEAD), jnp.float32)
        for j in range(PER_GROUP):
            rows = pl.ds(j * BLOCK, BLOCK)
            totals = jnp.sum(lbuf[rows, :], axis=-1, keepdims=True)
            head_out = (abuf[rows, :] / totals).astype(jnp.bfloat16)
            obuf[k, :, j * D_HEAD:(j + 1) * D_HEAD] = head_out
            direction = reward_dir[:, chunk * CHUNK + j * D_HEAD:chunk * CHUNK + (j + 1) * D_HEAD]
            scored += head_out.astype(jnp.float32) * direction
        score[k * BLOCK:(k + 1) * BLOCK, :] = scored
        pltpu.make_async_copy(
            obuf.at[k], out.at[pl.ds(k * BLOCK, BLOCK), columns], o_sems.at[k]
        ).start()
    for k in range(RECV):
        pltpu.make_async_copy(
            obuf.at[k], out.at[pl.ds(k * BLOCK, BLOCK), columns], o_sems.at[k]
        ).wait()


def attend(chunk, info, place, queries, q_left, q_right, window, reward_dir, previous, responses, ranks):
    capacity = queries.shape[0] // BLOCK
    smem = pl.BlockSpec(memory_space=pltpu.SMEM)
    anywhere = pl.BlockSpec(memory_space=pl.ANY)
    vmem = pl.BlockSpec(memory_space=pltpu.VMEM)
    operands = [info, place, queries, q_left, q_right, *window, reward_dir]
    in_specs = [smem, smem] + [anywhere] * 9 + [vmem]
    aliases = {}
    body = functools.partial(attend_kernel, responses, ranks, capacity, chunk)
    if previous is not None:
        aliases = {len(operands): 0}
        operands.append(previous)
        in_specs.append(anywhere)
        first = len(operands) - 1

        def body(*refs):
            kept = refs[:first] + refs[first + 1:]
            attend_kernel(responses, ranks, capacity, chunk, *kept)

    stacked = PER_GROUP * BLOCK
    return pl.pallas_call(
        body,
        out_shape=(
            jax.ShapeDtypeStruct((ROWS, HEADS * D_HEAD), jnp.bfloat16),
            jax.ShapeDtypeStruct((ROWS, D_HEAD), jnp.float32),
        ),
        in_specs=in_specs,
        out_specs=(anywhere, vmem),
        scratch_shapes=[
            pltpu.VMEM((PIECES, ROWS, D_HEAD), jnp.bfloat16),
            pltpu.VMEM((PIECES, ROWS, D_HEAD), jnp.bfloat16),
            pltpu.VMEM((RECV, BLOCK, CHUNK), jnp.bfloat16),
            pltpu.VMEM((RECV, BLOCK, CHUNK), jnp.bfloat16),
            pltpu.VMEM((PIECES, stacked, ROWS), jnp.float32),
            pltpu.VMEM((stacked, D_HEAD), jnp.float32),
            pltpu.VMEM((stacked, D_HEAD), jnp.float32),
            pltpu.VMEM((stacked, D_HEAD), jnp.float32),
            pltpu.SemaphoreType.DMA((RECV, 3)),
            pltpu.SemaphoreType.DMA((PIECES, 2)),
            pltpu.SemaphoreType.DMA((RECV,)),
        ],
        input_output_aliases=aliases,
        compiler_params=pltpu.CompilerParams(vmem_limit_bytes=24 * 1024 * 1024),
        cost_estimate=pl.CostEstimate(
            flops=4 * RECV * stacked * PIECES * ROWS * D_HEAD,
            bytes_accessed=4 * 1024 * 1024,
            transcendentals=RECV * stacked * PIECES * ROWS,
        ),
        name=f"attend_{chunk}",
    )(*operands)


def shards(queries, keys, values, block_counts, segment_ids, reward_dir):
    ranks = lax.axis_size("dp")
    rank = lax.axis_index("dp")
    row_count = segment_ids.shape[0]
    capacity = queries.shape[0] // BLOCK
    responses = ranks * 2 // REACH
    count = block_counts[0]

    tail = jnp.clip(count - RECV, 0, capacity - RECV) * BLOCK

    def tail_of(array, column, width):
        return lax.dynamic_slice(array, (tail, column), (row_count, width))

    kv_tail = jnp.concatenate([tail_of(keys, 0, KV_WIDTH), tail_of(values, 0, KV_WIDTH)], axis=1)
    kv_head = jnp.concatenate([keys[:row_count], values[:row_count]], axis=1)
    kv_left = shifted(kv_tail, "dp", 1)
    kv_right = shifted(kv_head, "dp", -1)
    q_left, q_right = [], []
    for chunk in range(KV_HEADS):
        q_left.append(shifted(tail_of(queries, chunk * CHUNK, CHUNK), "dp", 1))
        q_right.append(
            shifted(queries[:row_count, chunk * CHUNK:(chunk + 1) * CHUNK], "dp", -1)
        )

    ids = jnp.arange(responses, dtype=jnp.int32)
    smaller = jnp.sum((segment_ids[None, :] < ids[:, None]).astype(jnp.int32), axis=1)
    marks = jnp.where(jnp.arange(ranks, dtype=jnp.int32) == rank, count, 0)
    info = lax.psum(jnp.concatenate([smaller, marks]), "dp")
    place = rank.astype(jnp.int32).reshape(1)

    own = pack(info, place, keys, values, kv_left, kv_right, responses, ranks)
    two = shifted(own, "dp", 2)
    four = shifted(own, "dp", 4)
    pairs = range(ranks // 2)
    sib_own = lax.ppermute(own, "dp", [(2 * m, 2 * m + 1) for m in pairs])
    sib_two = lax.ppermute(two, "dp", [(i, i ^ 1) for i in range(ranks)])
    sib_four = lax.ppermute(four, "dp", [(2 * m + 1, 2 * m) for m in pairs])
    window = (own, two, four, sib_own, sib_two, sib_four)

    direction = reward_dir.reshape(1, -1)
    attn_out, scores = None, []
    for chunk in range(KV_HEADS):
        attn_out, score = attend(
            chunk, info, place, queries, q_left[chunk], q_right[chunk], window, direction,
            attn_out, responses, ranks,
        )
        scores.append(score)
    token_score = jnp.sum(sum(scores), axis=1)
    ends = jnp.concatenate([info[1:responses], jnp.full((1,), ranks * row_count, jnp.int32)])
    positions = rank * row_count + jnp.arange(row_count, dtype=jnp.int32)
    matches = positions[None, :] == ends[:, None] - 1
    partial_rewards = jnp.sum(jnp.where(matches, token_score[None, :], 0.0), axis=1)
    rewards = lax.psum(partial_rewards, "dp")
    return (attn_out, rewards)


def solution(mesh):
    return jax.shard_map(
        shards,
        mesh=mesh,
        in_specs=(
            P(("groups", "dp"), None),
            P(("groups", "dp"), None),
            P(("groups", "dp"), None),
            P(("groups", "dp")),
            P(("groups", "dp")),
            P(),
        ),
        out_specs=(P(("groups", "dp"), None), P("groups")),
        check_vma=False,
    )
```

```python
import functools
import math

import jax
import jax.numpy as jnp
from jax import lax
from jax.experimental import pallas as pl
from jax.experimental.pallas import tpu as pltpu
from jax.sharding import PartitionSpec as P

D_HEAD = 128
HEADS = 32
KV_HEADS = 4
BLOCK = 128
RECV = 2
REACH = 4
PER_GROUP = HEADS // KV_HEADS
ROWS = RECV * BLOCK
PIECES = REACH + 1
KV_WIDTH = KV_HEADS * D_HEAD
WIDTH = HEADS * D_HEAD
CHUNK = PER_GROUP * D_HEAD
STACKED = PER_GROUP * BLOCK
PAIR = 2
MASKED = -1e30
WIDE = pltpu.CompilerParams(vmem_limit_bytes=58 * 1024 * 1024 + 256 * 1024)
SLIM = pltpu.CompilerParams(vmem_limit_bytes=28 * 1024 * 1024)
EXP2_SCALE = D_HEAD ** (-0.5) * math.log2(math.e)
SPLIT = ((0,), (1, 2), (3,))

SMEM = pl.BlockSpec(memory_space=pltpu.SMEM)
VMEM = pl.BlockSpec(memory_space=pltpu.VMEM)
HBM = pl.BlockSpec(memory_space=pltpu.HBM)


def shifted(block, axis, distance):
    devices = range(lax.axis_size(axis))
    route = [(i - distance, i) for i in devices if i - distance in devices]
    return lax.ppermute(block, axis, route)


def inner_pairs(block, ranks):
    return lax.ppermute(block, "dp", [(i, i ^ 1) for i in range(ranks)])


def outer_pairs(block, ranks):
    route = []
    for low in range(1, ranks - 1, 2):
        route += [(low, low + 1), (low + 1, low)]
    return lax.ppermute(block, "dp", route)


def block_rows(index):
    return pl.ds(pl.multiple_of(index * BLOCK, BLOCK), BLOCK)


def columns_of(heads):
    return pl.ds(heads[0] * CHUNK, len(heads) * CHUNK)


def transfer(copies):
    for copy in copies:
        copy.start()
    for copy in copies:
        copy.wait()


def end_rows(counts, place, capacity):
    tail = jnp.clip(counts[0] - RECV, 0, capacity - RECV) * BLOCK
    odd = lax.rem(place[0], 2) == 1
    outer = pl.multiple_of(jnp.where(odd, tail, 0), BLOCK)
    inner = pl.multiple_of(jnp.where(odd, 0, tail), BLOCK)
    return pl.ds(outer, ROWS), pl.ds(inner, ROWS)


def first_stage_kernel(capacity, counts, place, queries, keys, values, kv_outer, kv_inner, q_outer, sems):
    outer, inner = end_rows(counts, place, capacity)
    key_part, value_part = pl.ds(0, KV_WIDTH), pl.ds(KV_WIDTH, KV_WIDTH)
    transfer([
        pltpu.make_async_copy(keys.at[outer], kv_outer.at[:, key_part], sems.at[0]),
        pltpu.make_async_copy(values.at[outer], kv_outer.at[:, value_part], sems.at[1]),
        pltpu.make_async_copy(keys.at[inner], kv_inner.at[:, key_part], sems.at[2]),
        pltpu.make_async_copy(values.at[inner], kv_inner.at[:, value_part], sems.at[3]),
        pltpu.make_async_copy(queries.at[outer, columns_of(SPLIT[0])], q_outer, sems.at[4]),
    ])


def first_stage(counts, place, queries, keys, values):
    capacity = queries.shape[0] // BLOCK
    kv = jax.ShapeDtypeStruct((ROWS, 2 * KV_WIDTH), keys.dtype)
    q = jax.ShapeDtypeStruct((ROWS, len(SPLIT[0]) * CHUNK), queries.dtype)
    return pl.pallas_call(
        functools.partial(first_stage_kernel, capacity),
        out_shape=(kv, kv, q),
        in_specs=[SMEM, SMEM, HBM, HBM, HBM],
        out_specs=(VMEM, VMEM, VMEM),
        scratch_shapes=[pltpu.SemaphoreType.DMA((5,))],
        compiler_params=WIDE,
        name="first_stage",
    )(counts, place, queries, keys, values)


def second_stage_kernel(capacity, counts, place, queries, *rest):
    outs, sems = rest[:-1], rest[-1]
    outer, inner = end_rows(counts, place, capacity)
    copies = [
        pltpu.make_async_copy(queries.at[outer, columns_of(heads)], out, sems.at[i])
        for i, (heads, out) in enumerate(zip(SPLIT[1:], outs))
    ]
    copies.append(pltpu.make_async_copy(queries.at[inner], outs[-1], sems.at[len(SPLIT) - 1]))
    transfer(copies)


def second_stage(counts, place, queries):
    capacity = queries.shape[0] // BLOCK
    widths = [len(heads) * CHUNK for heads in SPLIT[1:]] + [WIDTH]
    return pl.pallas_call(
        functools.partial(second_stage_kernel, capacity),
        out_shape=tuple(jax.ShapeDtypeStruct((ROWS, width), queries.dtype) for width in widths),
        in_specs=[SMEM, SMEM, HBM],
        out_specs=(VMEM,) * len(widths),
        scratch_shapes=[pltpu.SemaphoreType.DMA((len(SPLIT),))],
        compiler_params=WIDE,
        name="second_stage",
    )(counts, place, queries)


def placement(info, place, responses, ranks):
    rank = place[0]
    before = lax.fori_loop(
        0, ranks, lambda s, t: t + jnp.where(s < rank, info[responses + s], 0), jnp.int32(0)
    )
    left_count = info[responses + jnp.maximum(rank - 1, 0)]
    return rank, before - rank * RECV, info[responses + rank], left_count


def pick(k, rank, excess, count, left_count, capacity):
    left_first = jnp.clip(left_count - RECV, 0, capacity - RECV)
    from_left = k < excess
    slot = k - excess
    is_own = jnp.logical_and(jnp.logical_not(from_left), slot < count)
    odd = lax.rem(rank, 2)
    left_kind, right_kind = jnp.where(odd == 1, 2, 0), jnp.where(odd == 1, 0, 2)
    kind = jnp.where(from_left, left_kind, jnp.where(is_own, 1, right_kind))
    index = jnp.where(
        from_left, left_count - excess + k - left_first, jnp.where(is_own, slot, slot - count)
    )
    limit = jnp.where(is_own, capacity - 1, RECV - 1)
    return kind, jnp.clip(index, 0, limit)


def pack_kernel(
    responses, ranks, capacity,
    info, place, queries, keys, values, outer, inner,
    out, q_own, sems,
):
    rank, excess, count, left_count = placement(info, place, responses, ranks)
    picks = [pick(k, rank, excess, count, left_count, capacity) for k in range(RECV)]
    jobs = []
    key_part, value_part = pl.ds(0, KV_WIDTH), pl.ds(KV_WIDTH, KV_WIDTH)
    for k, (kind, index) in enumerate(picks):
        rows = block_rows(index)
        into = pl.ds(k * BLOCK, BLOCK)
        mine = kind == 1
        jobs += [
            (mine, pltpu.make_async_copy(keys.at[rows], out.at[into, key_part], sems.at[k, 0])),
            (mine, pltpu.make_async_copy(values.at[rows], out.at[into, value_part], sems.at[k, 1])),
            (mine, pltpu.make_async_copy(queries.at[rows], q_own.at[into], sems.at[k, 2])),
        ]
    each(jobs, "start")

    for k, (kind, index) in enumerate(picks):
        for wanted, source in ((0, outer), (2, inner)):
            @pl.when(kind == wanted)
            def _(source=source, k=k, index=index):
                out[k * BLOCK:(k + 1) * BLOCK, :] = source[block_rows(index), :]
    each(jobs, "wait")


def pack(info, place, queries, keys, values, outer, inner, responses, ranks):
    capacity = keys.shape[0] // BLOCK
    return pl.pallas_call(
        functools.partial(pack_kernel, responses, ranks, capacity),
        out_shape=(
            jax.ShapeDtypeStruct((ROWS, 2 * KV_WIDTH), keys.dtype),
            jax.ShapeDtypeStruct((ROWS, WIDTH), queries.dtype),
        ),
        in_specs=[SMEM, SMEM, HBM, HBM, HBM, VMEM, VMEM],
        out_specs=(VMEM, VMEM),
        scratch_shapes=[
            pltpu.SemaphoreType.DMA((RECV, 3)),
        ],
        compiler_params=WIDE,
        name="pack",
    )(info, place, queries, keys, values, outer, inner)


def fill_window(rank, window, head, lowest, kbuf, vbuf):
    own, two, four, sib_own, sib_two, sib_four = window
    odd = lax.rem(rank, 2) == 1
    even = jnp.logical_not(odd)
    sources = ((None, own, 4), (odd, sib_own, 3), (even, sib_two, 3), (None, two, 2),
               (odd, sib_two, 1), (even, sib_four, 1), (None, four, 0))
    for condition, source, piece in sources:
        needed = lowest <= piece
        if condition is not None:
            needed = jnp.logical_and(needed, condition)

        @pl.when(needed)
        def _(source=source, piece=piece):
            kbuf[piece] = source[:, head * D_HEAD:(head + 1) * D_HEAD]
            vbuf[piece] = source[:, KV_WIDTH + head * D_HEAD:KV_WIDTH + (head + 1) * D_HEAD]


def each(jobs, action):
    for condition, copy in jobs:
        if condition is None:
            getattr(copy, action)()
        else:
            pl.when(condition)(getattr(copy, action))


def attend_kernel(
    responses, ranks, capacity, heads, earlier, rewards,
    info, place, q_own, q_outer, q_inner, own, two, four, sib_own, sib_two, sib_four,
    reward_dir, out, score, kbuf, vbuf, qbuf, obuf, sbuf, mbuf, lbuf, abuf, o_sems,
):
    rank, excess, count, left_count = placement(info, place, responses, ranks)
    columns = slice(heads[0] * CHUNK, (heads[-1] + 1) * CHUNK)
    for k in range(RECV):
        kind, index = pick(k, rank, excess, count, left_count, capacity)

        @pl.when(kind == 0)
        def _(k=k, index=index):
            qbuf[k] = q_outer[block_rows(index), :]

        @pl.when(kind == 1)
        def _(k=k):
            qbuf[k] = q_own[k * BLOCK:(k + 1) * BLOCK, columns]

        @pl.when(kind == 2)
        def _(k=k, index=index):
            qbuf[k] = q_inner[block_rows(index), columns]

    window = (own, two, four, sib_own, sib_two, sib_four)
    window_base = (rank - REACH) * ROWS
    first = rank * ROWS
    row_iota = lax.broadcasted_iota(jnp.int32, (ROWS, D_HEAD), 0)
    lane_iota = lax.broadcasted_iota(jnp.int32, (BLOCK, D_HEAD), 1)
    rows_at = row_iota + first

    def widen(r, carry):
        begin, begins = carry
        start = info[r]
        begin = jnp.where(start <= first, jnp.maximum(begin, start), begin)
        begins = jnp.where(rows_at >= start, jnp.maximum(begins, start), begins)
        return begin, begins

    begin, begins = lax.fori_loop(
        0, responses, widen, (jnp.int32(0), jnp.zeros((ROWS, D_HEAD), jnp.int32))
    )
    lowest = jnp.clip((begin - window_base) // ROWS, 0, REACH)

    stores = []
    score[...] = jnp.zeros_like(score)
    for at, head in enumerate(heads):
        fill_window(rank, window, head, lowest, kbuf, vbuf)
        mbuf[...] = jnp.full_like(mbuf, MASKED)

        def score_tile(p, _):
            base = window_base + p * ROWS
            key_tile = kbuf[p]
            for k in range(RECV):
                block = slice(k * BLOCK, (k + 1) * BLOCK)
                masks = []
                for half in range(2):
                    key_at = lane_iota + (base + half * D_HEAD)
                    masks.append(jnp.logical_and(key_at >= begins[block], key_at <= rows_at[block]))
                for j in range(0, PER_GROUP, PAIR):
                    parts = [
                        qbuf[k, :, at * CHUNK + i * D_HEAD:at * CHUNK + (i + 1) * D_HEAD]
                        for i in range(j, j + PAIR)
                    ]
                    logits = lax.dot_general(
                        jnp.concatenate(parts, axis=0), key_tile, (((1,), (1,)), ((), ())),
                        preferred_element_type=jnp.float32,
                    )
                    for i in range(PAIR):
                        rows = pl.ds(k * STACKED + (j + i) * BLOCK, BLOCK)
                        part = logits[i * BLOCK:(i + 1) * BLOCK]
                        low = jnp.where(masks[0], part[:, :D_HEAD], MASKED)
                        high = jnp.where(masks[1], part[:, D_HEAD:], MASKED)
                        sbuf[p, rows, :D_HEAD] = low
                        sbuf[p, rows, D_HEAD:] = high
                        mbuf[rows, :] = jnp.maximum(mbuf[rows, :], jnp.maximum(low, high))
            return 0

        lax.fori_loop(lowest, PIECES, score_tile, 0)
        for i in range(RECV * PER_GROUP):
            rows = pl.ds(i * BLOCK, BLOCK)
            peak = jnp.max(mbuf[rows, :], axis=-1, keepdims=True)
            mbuf[rows, :] = jnp.broadcast_to(peak, (BLOCK, D_HEAD))
        lbuf[...] = jnp.zeros_like(lbuf)
        abuf[...] = jnp.zeros_like(abuf)

        def weigh_tile(p, _):
            value_tile = vbuf[p]
            for i in range(0, RECV * PER_GROUP, PAIR):
                rows = pl.ds(i * BLOCK, PAIR * BLOCK)
                peak = mbuf[rows, :]
                low = jnp.exp2((sbuf[p, rows, :D_HEAD] - peak) * EXP2_SCALE)
                high = jnp.exp2((sbuf[p, rows, D_HEAD:] - peak) * EXP2_SCALE)
                lbuf[rows, :] += low + high
                soft = jnp.concatenate([low.astype(jnp.bfloat16), high.astype(jnp.bfloat16)], axis=1)
                abuf[rows, :] += jnp.dot(soft, value_tile, preferred_element_type=jnp.float32)
            return 0

        lax.fori_loop(lowest, PIECES, weigh_tile, 0)
        for k in range(RECV):
            scored = score[k * BLOCK:(k + 1) * BLOCK, :]
            for j in range(PER_GROUP):
                rows = pl.ds(k * STACKED + j * BLOCK, BLOCK)
                totals = jnp.sum(lbuf[rows, :], axis=-1, keepdims=True)
                into = slice(at * CHUNK + j * D_HEAD, at * CHUNK + (j + 1) * D_HEAD)
                head_out = (abuf[rows, :] / totals).astype(jnp.bfloat16)
                obuf[k, :, into] = head_out
                direction = reward_dir[:, head * CHUNK + j * D_HEAD:head * CHUNK + (j + 1) * D_HEAD]
                scored += head_out.astype(jnp.float32) * direction
            score[k * BLOCK:(k + 1) * BLOCK, :] = scored
            store = pltpu.make_async_copy(
                obuf.at[k, :, pl.ds(at * CHUNK, CHUNK)],
                out.at[pl.ds(k * BLOCK, BLOCK), pl.ds(head * CHUNK, CHUNK)],
                o_sems.at[at, k],
            )
            store.start()
            stores.append(store)
    if earlier:
        score[...] += sum(part[...] for part in earlier)
    if rewards is not None:
        def settle(r, _):
            following = info[jnp.minimum(r + 1, responses - 1)]
            at = jnp.where(r + 1 < responses, following, ranks * ROWS) - 1 - first
            here = jnp.logical_and(at >= 0, at < ROWS)
            row = score[pl.ds(jnp.clip(at, 0, ROWS - 1), 1), :]
            rewards[pl.ds(r, 1), :] = jnp.where(here, row, 0.0)
            return 0

        lax.fori_loop(0, responses, settle, 0)
    for store in stores:
        store.wait()


def attend(
    heads, info, place, q_own, q_outer, q_inner, window, reward_dir, previous, scores, last,
    capacity, responses, ranks,
):
    operands = [info, place, q_own, q_outer, q_inner, *window, reward_dir]
    used = len(operands)
    in_specs = [SMEM, SMEM] + [VMEM] * 10
    aliases = {}
    if previous is not None:
        aliases = {used: 0}
        operands += [previous] + scores
        in_specs += [HBM] + [VMEM] * len(scores)
    taken = len(operands)
    out_shape = [
        jax.ShapeDtypeStruct((ROWS, WIDTH), jnp.bfloat16),
        jax.ShapeDtypeStruct((ROWS, D_HEAD), jnp.float32),
    ]
    if last:
        out_shape.append(jax.ShapeDtypeStruct((responses, D_HEAD), jnp.float32))
    made = taken + len(out_shape)

    def body(*refs):
        attend_kernel(
            responses, ranks, capacity, heads, refs[used + 1:taken], refs[made - 1] if last else None,
            *refs[:used], *refs[taken:taken + 2], *refs[made:],
        )

    number = len(heads)
    return pl.pallas_call(
        body,
        out_shape=out_shape,
        in_specs=in_specs,
        out_specs=[HBM] + [VMEM] * (len(out_shape) - 1),
        scratch_shapes=[
            pltpu.VMEM((PIECES, ROWS, D_HEAD), jnp.bfloat16),
            pltpu.VMEM((PIECES, ROWS, D_HEAD), jnp.bfloat16),
            pltpu.VMEM((RECV, BLOCK, number * CHUNK), jnp.bfloat16),
            pltpu.VMEM((RECV, BLOCK, number * CHUNK), jnp.bfloat16),
            pltpu.VMEM((PIECES, RECV * STACKED, ROWS), jnp.float32),
            pltpu.VMEM((RECV * STACKED, D_HEAD), jnp.float32),
            pltpu.VMEM((RECV * STACKED, D_HEAD), jnp.float32),
            pltpu.VMEM((RECV * STACKED, D_HEAD), jnp.float32),
            pltpu.SemaphoreType.DMA((number, RECV)),
        ],
        input_output_aliases=aliases,
        compiler_params=SLIM,
        cost_estimate=pl.CostEstimate(
            flops=4 * number * RECV * STACKED * PIECES * ROWS * D_HEAD,
            bytes_accessed=2 * number * 1024 * 1024,
            transcendentals=number * RECV * STACKED * PIECES * ROWS,
        ),
    )(*operands)


def shards(queries, keys, values, block_counts, segment_ids, reward_dir):
    ranks = lax.axis_size("dp")
    rank = lax.axis_index("dp")
    capacity = queries.shape[0] // BLOCK
    responses = ranks * 2 // REACH
    place = rank.astype(jnp.int32).reshape(1)

    kv_outer, kv_inner, q_first = first_stage(block_counts, place, queries, keys, values)
    kv_outer = outer_pairs(kv_outer, ranks)
    kv_inner = inner_pairs(kv_inner, ranks)
    q_outer = [outer_pairs(q_first, ranks)]

    ids = jnp.arange(responses, dtype=jnp.int32)
    smaller = jnp.sum((segment_ids[None, :] < ids[:, None]).astype(jnp.int32), axis=1)
    marks = jnp.where(jnp.arange(ranks, dtype=jnp.int32) == rank, block_counts[0], 0)
    info = lax.psum(jnp.concatenate([smaller, marks]), "dp")

    own, q_own = pack(info, place, queries, keys, values, kv_outer, kv_inner, responses, ranks)
    two = shifted(own, "dp", 2)
    four = shifted(own, "dp", 4)
    pairs = range(ranks // 2)
    sib_own = lax.ppermute(own, "dp", [(2 * m, 2 * m + 1) for m in pairs])

    *q_later, q_inner = second_stage(block_counts, place, queries)
    for part in q_later:
        q_outer.append(outer_pairs(part, ranks))
    q_inner = inner_pairs(q_inner, ranks)

    sib_two = inner_pairs(two, ranks)
    sib_four = lax.ppermute(four, "dp", [(2 * m + 1, 2 * m) for m in pairs])
    window = (own, two, four, sib_own, sib_two, sib_four)

    direction = reward_dir.reshape(1, -1)
    attn_out, scores = None, []
    for i, heads in enumerate(SPLIT):
        last = i == len(SPLIT) - 1
        attn_out, score, *settled = attend(
            heads, info, place, q_own, q_outer[i], q_inner, window, direction, attn_out, scores,
            last, capacity, responses, ranks,
        )
        scores = [score]
    rewards = lax.psum(jnp.sum(settled[0], axis=1), "dp")
    return (attn_out, rewards)


def solution(mesh):
    return jax.shard_map(
        shards,
        mesh=mesh,
        in_specs=(
            P(("groups", "dp"), None),
            P(("groups", "dp"), None),
            P(("groups", "dp"), None),
            P(("groups", "dp")),
            P(("groups", "dp")),
            P(),
        ),
        out_specs=(P(("groups", "dp"), None), P("groups")),
        check_vma=False,
    )
```

```python
import functools
import math

import jax
import jax.numpy as jnp
from jax import lax
from jax.experimental import pallas as pl
from jax.experimental.pallas import tpu as pltpu
from jax.sharding import PartitionSpec as P

D_HEAD = 128
HEADS = 32
KV_HEADS = 4
BLOCK = 128
RECV = 2
REACH = 4
PER_GROUP = HEADS // KV_HEADS
ROWS = RECV * BLOCK
PIECES = REACH + 1
KV_WIDTH = KV_HEADS * D_HEAD
WIDTH = HEADS * D_HEAD
CHUNK = PER_GROUP * D_HEAD
STACKED = PER_GROUP * BLOCK
PAIR = 2
MASKED = -1e30
WIDE = pltpu.CompilerParams(vmem_limit_bytes=58 * 1024 * 1024 + 256 * 1024)
SLIM = pltpu.CompilerParams(vmem_limit_bytes=28 * 1024 * 1024)
EXP2_SCALE = D_HEAD ** (-0.5) * math.log2(math.e)
SPLIT = ((0,), (1, 2), (3,))

SMEM = pl.BlockSpec(memory_space=pltpu.SMEM)
VMEM = pl.BlockSpec(memory_space=pltpu.VMEM)
HBM = pl.BlockSpec(memory_space=pltpu.HBM)


def shifted(block, axis, distance):
    devices = range(lax.axis_size(axis))
    route = [(i - distance, i) for i in devices if i - distance in devices]
    return lax.ppermute(block, axis, route)


def inner_pairs(block, ranks):
    return lax.ppermute(block, "dp", [(i, i ^ 1) for i in range(ranks)])


def outer_pairs(block, ranks):
    route = []
    for low in range(1, ranks - 1, 2):
        route += [(low, low + 1), (low + 1, low)]
    return lax.ppermute(block, "dp", route)


def total_over(part, ranks):
    if ranks & (ranks - 1):
        return lax.psum(part, "dp")
    bit = 1
    while bit < ranks:
        part = part + lax.ppermute(part, "dp", [(i, i ^ bit) for i in range(ranks)])
        bit *= 2
    return part


def block_rows(index):
    return pl.ds(pl.multiple_of(index * BLOCK, BLOCK), BLOCK)


def columns_of(heads):
    return pl.ds(heads[0] * CHUNK, len(heads) * CHUNK)


def transfer(copies):
    for copy in copies:
        copy.start()
    for copy in copies:
        copy.wait()


def end_rows(counts, place, capacity):
    tail = jnp.clip(counts[0] - RECV, 0, capacity - RECV) * BLOCK
    odd = lax.rem(place[0], 2) == 1
    outer = pl.multiple_of(jnp.where(odd, tail, 0), BLOCK)
    inner = pl.multiple_of(jnp.where(odd, 0, tail), BLOCK)
    return pl.ds(outer, ROWS), pl.ds(inner, ROWS)


def first_stage_kernel(capacity, counts, place, queries, keys, values, kv_outer, kv_inner, q_outer, sems):
    outer, inner = end_rows(counts, place, capacity)
    key_part, value_part = pl.ds(0, KV_WIDTH), pl.ds(KV_WIDTH, KV_WIDTH)
    transfer([
        pltpu.make_async_copy(keys.at[outer], kv_outer.at[:, key_part], sems.at[0]),
        pltpu.make_async_copy(values.at[outer], kv_outer.at[:, value_part], sems.at[1]),
        pltpu.make_async_copy(keys.at[inner], kv_inner.at[:, key_part], sems.at[2]),
        pltpu.make_async_copy(values.at[inner], kv_inner.at[:, value_part], sems.at[3]),
        pltpu.make_async_copy(queries.at[outer, columns_of(SPLIT[0])], q_outer, sems.at[4]),
    ])


def first_stage(counts, place, queries, keys, values):
    capacity = queries.shape[0] // BLOCK
    kv = jax.ShapeDtypeStruct((ROWS, 2 * KV_WIDTH), keys.dtype)
    q = jax.ShapeDtypeStruct((ROWS, len(SPLIT[0]) * CHUNK), queries.dtype)
    return pl.pallas_call(
        functools.partial(first_stage_kernel, capacity),
        out_shape=(kv, kv, q),
        in_specs=[SMEM, SMEM, HBM, HBM, HBM],
        out_specs=(VMEM, VMEM, VMEM),
        scratch_shapes=[pltpu.SemaphoreType.DMA((5,))],
        compiler_params=WIDE,
        name="first_stage",
    )(counts, place, queries, keys, values)


def second_stage_kernel(capacity, counts, place, queries, *rest):
    outs, sems = rest[:-1], rest[-1]
    outer, inner = end_rows(counts, place, capacity)
    copies = [
        pltpu.make_async_copy(queries.at[outer, columns_of(heads)], out, sems.at[i])
        for i, (heads, out) in enumerate(zip(SPLIT[1:], outs))
    ]
    copies.append(pltpu.make_async_copy(queries.at[inner], outs[-1], sems.at[len(SPLIT) - 1]))
    transfer(copies)


def second_stage(counts, place, queries):
    capacity = queries.shape[0] // BLOCK
    widths = [len(heads) * CHUNK for heads in SPLIT[1:]] + [WIDTH]
    return pl.pallas_call(
        functools.partial(second_stage_kernel, capacity),
        out_shape=tuple(jax.ShapeDtypeStruct((ROWS, width), queries.dtype) for width in widths),
        in_specs=[SMEM, SMEM, HBM],
        out_specs=(VMEM,) * len(widths),
        scratch_shapes=[pltpu.SemaphoreType.DMA((len(SPLIT),))],
        compiler_params=WIDE,
        name="second_stage",
    )(counts, place, queries)


def placement(info, place, responses, ranks):
    rank = place[0]
    before = lax.fori_loop(
        0, ranks, lambda s, t: t + jnp.where(s < rank, info[responses + s], 0), jnp.int32(0)
    )
    left_count = info[responses + jnp.maximum(rank - 1, 0)]
    return rank, before - rank * RECV, info[responses + rank], left_count


def pick(k, rank, excess, count, left_count, capacity):
    left_first = jnp.clip(left_count - RECV, 0, capacity - RECV)
    from_left = k < excess
    slot = k - excess
    is_own = jnp.logical_and(jnp.logical_not(from_left), slot < count)
    odd = lax.rem(rank, 2)
    left_kind, right_kind = jnp.where(odd == 1, 2, 0), jnp.where(odd == 1, 0, 2)
    kind = jnp.where(from_left, left_kind, jnp.where(is_own, 1, right_kind))
    index = jnp.where(
        from_left, left_count - excess + k - left_first, jnp.where(is_own, slot, slot - count)
    )
    limit = jnp.where(is_own, capacity - 1, RECV - 1)
    return kind, jnp.clip(index, 0, limit)


def pack_kernel(
    responses, ranks, capacity,
    info, place, queries, keys, values, outer, inner,
    out, q_own, sems,
):
    rank, excess, count, left_count = placement(info, place, responses, ranks)
    picks = [pick(k, rank, excess, count, left_count, capacity) for k in range(RECV)]
    jobs = []
    key_part, value_part = pl.ds(0, KV_WIDTH), pl.ds(KV_WIDTH, KV_WIDTH)
    for k, (kind, index) in enumerate(picks):
        rows = block_rows(index)
        into = pl.ds(k * BLOCK, BLOCK)
        mine = kind == 1
        jobs += [
            (mine, pltpu.make_async_copy(keys.at[rows], out.at[into, key_part], sems.at[k, 0])),
            (mine, pltpu.make_async_copy(values.at[rows], out.at[into, value_part], sems.at[k, 1])),
            (mine, pltpu.make_async_copy(queries.at[rows], q_own.at[into], sems.at[k, 2])),
        ]
    each(jobs, "start")

    for k, (kind, index) in enumerate(picks):
        for wanted, source in ((0, outer), (2, inner)):
            @pl.when(kind == wanted)
            def _(source=source, k=k, index=index):
                out[k * BLOCK:(k + 1) * BLOCK, :] = source[block_rows(index), :]
    each(jobs, "wait")


def pack(info, place, queries, keys, values, outer, inner, responses, ranks):
    capacity = keys.shape[0] // BLOCK
    return pl.pallas_call(
        functools.partial(pack_kernel, responses, ranks, capacity),
        out_shape=(
            jax.ShapeDtypeStruct((ROWS, 2 * KV_WIDTH), keys.dtype),
            jax.ShapeDtypeStruct((ROWS, WIDTH), queries.dtype),
        ),
        in_specs=[SMEM, SMEM, HBM, HBM, HBM, VMEM, VMEM],
        out_specs=(VMEM, VMEM),
        scratch_shapes=[
            pltpu.SemaphoreType.DMA((RECV, 3)),
        ],
        compiler_params=WIDE,
        name="pack",
    )(info, place, queries, keys, values, outer, inner)


def fill_window(rank, window, head, lowest, kbuf, vbuf):
    own, two, four, sib_own, sib_two, sib_four = window
    odd = lax.rem(rank, 2) == 1
    even = jnp.logical_not(odd)
    sources = ((None, own, 4), (odd, sib_own, 3), (even, sib_two, 3), (None, two, 2),
               (odd, sib_two, 1), (even, sib_four, 1), (None, four, 0))
    for condition, source, piece in sources:
        needed = lowest <= piece
        if condition is not None:
            needed = jnp.logical_and(needed, condition)

        @pl.when(needed)
        def _(source=source, piece=piece):
            kbuf[piece] = source[:, head * D_HEAD:(head + 1) * D_HEAD]
            vbuf[piece] = source[:, KV_WIDTH + head * D_HEAD:KV_WIDTH + (head + 1) * D_HEAD]


def each(jobs, action):
    for condition, copy in jobs:
        if condition is None:
            getattr(copy, action)()
        else:
            pl.when(condition)(getattr(copy, action))


def attend_kernel(
    responses, ranks, capacity, heads, earlier, rewards,
    info, place, q_own, q_outer, q_inner, own, two, four, sib_own, sib_two, sib_four,
    reward_dir, out, score, kbuf, vbuf, qbuf, obuf, sbuf, mbuf, lbuf, abuf, o_sems,
):
    rank, excess, count, left_count = placement(info, place, responses, ranks)
    columns = slice(heads[0] * CHUNK, (heads[-1] + 1) * CHUNK)
    for k in range(RECV):
        kind, index = pick(k, rank, excess, count, left_count, capacity)

        @pl.when(kind == 0)
        def _(k=k, index=index):
            qbuf[k] = q_outer[block_rows(index), :]

        @pl.when(kind == 1)
        def _(k=k):
            qbuf[k] = q_own[k * BLOCK:(k + 1) * BLOCK, columns]

        @pl.when(kind == 2)
        def _(k=k, index=index):
            qbuf[k] = q_inner[block_rows(index), columns]

    window = (own, two, four, sib_own, sib_two, sib_four)
    window_base = (rank - REACH) * ROWS
    first = rank * ROWS
    row_iota = lax.broadcasted_iota(jnp.int32, (ROWS, D_HEAD), 0)
    lane_iota = lax.broadcasted_iota(jnp.int32, (BLOCK, D_HEAD), 1)
    rows_at = row_iota + first

    def widen(r, carry):
        begin, begins = carry
        start = info[r]
        begin = jnp.where(start <= first, jnp.maximum(begin, start), begin)
        begins = jnp.where(rows_at >= start, jnp.maximum(begins, start), begins)
        return begin, begins

    begin, begins = lax.fori_loop(
        0, responses, widen, (jnp.int32(0), jnp.zeros((ROWS, D_HEAD), jnp.int32))
    )
    lowest = jnp.clip((begin - window_base) // ROWS, 0, REACH)

    stores = []
    score[...] = jnp.zeros_like(score)
    for at, head in enumerate(heads):
        fill_window(rank, window, head, lowest, kbuf, vbuf)
        mbuf[...] = jnp.full_like(mbuf, MASKED)

        def score_tile(p, _):
            base = window_base + p * ROWS
            key_tile = kbuf[p]
            for k in range(RECV):
                block = slice(k * BLOCK, (k + 1) * BLOCK)
                masks = []
                for half in range(2):
                    key_at = lane_iota + (base + half * D_HEAD)
                    masks.append(jnp.logical_and(key_at >= begins[block], key_at <= rows_at[block]))
                for j in range(0, PER_GROUP, PAIR):
                    parts = [
                        qbuf[k, :, at * CHUNK + i * D_HEAD:at * CHUNK + (i + 1) * D_HEAD]
                        for i in range(j, j + PAIR)
                    ]
                    logits = lax.dot_general(
                        jnp.concatenate(parts, axis=0), key_tile, (((1,), (1,)), ((), ())),
                        preferred_element_type=jnp.float32,
                    )
                    for i in range(PAIR):
                        rows = pl.ds(k * STACKED + (j + i) * BLOCK, BLOCK)
                        part = logits[i * BLOCK:(i + 1) * BLOCK]
                        low = jnp.where(masks[0], part[:, :D_HEAD], MASKED)
                        high = jnp.where(masks[1], part[:, D_HEAD:], MASKED)
                        sbuf[p, rows, :D_HEAD] = low
                        sbuf[p, rows, D_HEAD:] = high
                        mbuf[rows, :] = jnp.maximum(mbuf[rows, :], jnp.maximum(low, high))
            return 0

        lax.fori_loop(lowest, PIECES, score_tile, 0)
        for i in range(RECV * PER_GROUP):
            rows = pl.ds(i * BLOCK, BLOCK)
            peak = jnp.max(mbuf[rows, :], axis=-1, keepdims=True)
            mbuf[rows, :] = jnp.broadcast_to(peak, (BLOCK, D_HEAD))
        lbuf[...] = jnp.zeros_like(lbuf)
        abuf[...] = jnp.zeros_like(abuf)

        def weigh_tile(p, _):
            value_tile = vbuf[p]
            for i in range(0, RECV * PER_GROUP, PAIR):
                rows = pl.ds(i * BLOCK, PAIR * BLOCK)
                peak = mbuf[rows, :]
                low = jnp.exp2((sbuf[p, rows, :D_HEAD] - peak) * EXP2_SCALE)
                high = jnp.exp2((sbuf[p, rows, D_HEAD:] - peak) * EXP2_SCALE)
                lbuf[rows, :] += low + high
                soft = jnp.concatenate([low.astype(jnp.bfloat16), high.astype(jnp.bfloat16)], axis=1)
                abuf[rows, :] += jnp.dot(soft, value_tile, preferred_element_type=jnp.float32)
            return 0

        lax.fori_loop(lowest, PIECES, weigh_tile, 0)
        for k in range(RECV):
            scored = score[k * BLOCK:(k + 1) * BLOCK, :]
            for j in range(PER_GROUP):
                rows = pl.ds(k * STACKED + j * BLOCK, BLOCK)
                totals = jnp.sum(lbuf[rows, :], axis=-1, keepdims=True)
                into = slice(at * CHUNK + j * D_HEAD, at * CHUNK + (j + 1) * D_HEAD)
                head_out = (abuf[rows, :] / totals).astype(jnp.bfloat16)
                obuf[k, :, into] = head_out
                direction = reward_dir[:, head * CHUNK + j * D_HEAD:head * CHUNK + (j + 1) * D_HEAD]
                scored += head_out.astype(jnp.float32) * direction
            score[k * BLOCK:(k + 1) * BLOCK, :] = scored
            store = pltpu.make_async_copy(
                obuf.at[k, :, pl.ds(at * CHUNK, CHUNK)],
                out.at[pl.ds(k * BLOCK, BLOCK), pl.ds(head * CHUNK, CHUNK)],
                o_sems.at[at, k],
            )
            store.start()
            stores.append(store)
    if earlier:
        score[...] += sum(part[...] for part in earlier)
    if rewards is not None:
        def settle(r, _):
            following = info[jnp.minimum(r + 1, responses - 1)]
            at = jnp.where(r + 1 < responses, following, ranks * ROWS) - 1 - first
            here = jnp.logical_and(at >= 0, at < ROWS)
            row = score[pl.ds(jnp.clip(at, 0, ROWS - 1), 1), :]
            rewards[pl.ds(r, 1), :] = jnp.where(here, row, 0.0)
            return 0

        lax.fori_loop(0, responses, settle, 0)
    for store in stores:
        store.wait()


def attend(
    heads, info, place, q_own, q_outer, q_inner, window, reward_dir, previous, scores, last,
    capacity, responses, ranks,
):
    operands = [info, place, q_own, q_outer, q_inner, *window, reward_dir]
    used = len(operands)
    in_specs = [SMEM, SMEM] + [VMEM] * 10
    aliases = {}
    if previous is not None:
        aliases = {used: 0}
        operands += [previous] + scores
        in_specs += [HBM] + [VMEM] * len(scores)
    taken = len(operands)
    out_shape = [
        jax.ShapeDtypeStruct((ROWS, WIDTH), jnp.bfloat16),
        jax.ShapeDtypeStruct((ROWS, D_HEAD), jnp.float32),
    ]
    if last:
        out_shape.append(jax.ShapeDtypeStruct((responses, D_HEAD), jnp.float32))
    made = taken + len(out_shape)

    def body(*refs):
        attend_kernel(
            responses, ranks, capacity, heads, refs[used + 1:taken], refs[made - 1] if last else None,
            *refs[:used], *refs[taken:taken + 2], *refs[made:],
        )

    number = len(heads)
    return pl.pallas_call(
        body,
        out_shape=out_shape,
        in_specs=in_specs,
        out_specs=[HBM] + [VMEM] * (len(out_shape) - 1),
        scratch_shapes=[
            pltpu.VMEM((PIECES, ROWS, D_HEAD), jnp.bfloat16),
            pltpu.VMEM((PIECES, ROWS, D_HEAD), jnp.bfloat16),
            pltpu.VMEM((RECV, BLOCK, number * CHUNK), jnp.bfloat16),
            pltpu.VMEM((RECV, BLOCK, number * CHUNK), jnp.bfloat16),
            pltpu.VMEM((PIECES, RECV * STACKED, ROWS), jnp.float32),
            pltpu.VMEM((RECV * STACKED, D_HEAD), jnp.float32),
            pltpu.VMEM((RECV * STACKED, D_HEAD), jnp.float32),
            pltpu.VMEM((RECV * STACKED, D_HEAD), jnp.float32),
            pltpu.SemaphoreType.DMA((number, RECV)),
        ],
        input_output_aliases=aliases,
        compiler_params=SLIM,
        cost_estimate=pl.CostEstimate(
            flops=4 * number * RECV * STACKED * PIECES * ROWS * D_HEAD,
            bytes_accessed=2 * number * 1024 * 1024,
            transcendentals=number * RECV * STACKED * PIECES * ROWS,
        ),
    )(*operands)


def shards(queries, keys, values, block_counts, segment_ids, reward_dir):
    ranks = lax.axis_size("dp")
    rank = lax.axis_index("dp")
    capacity = queries.shape[0] // BLOCK
    responses = ranks * 2 // REACH
    place = rank.astype(jnp.int32).reshape(1)

    kv_outer, kv_inner, q_first = first_stage(block_counts, place, queries, keys, values)
    kv_outer = outer_pairs(kv_outer, ranks)
    kv_inner = inner_pairs(kv_inner, ranks)
    q_outer = [outer_pairs(q_first, ranks)]

    ids = jnp.arange(responses, dtype=jnp.int32)
    smaller = jnp.sum((segment_ids[None, :] < ids[:, None]).astype(jnp.int32), axis=1)
    marks = jnp.where(jnp.arange(ranks, dtype=jnp.int32) == rank, block_counts[0], 0)
    info = lax.psum(jnp.concatenate([smaller, marks]), "dp")

    own, q_own = pack(info, place, queries, keys, values, kv_outer, kv_inner, responses, ranks)
    two = shifted(own, "dp", 2)
    four = shifted(own, "dp", 4)
    pairs = range(ranks // 2)
    sib_own = lax.ppermute(own, "dp", [(2 * m, 2 * m + 1) for m in pairs])

    *q_later, q_inner = second_stage(block_counts, place, queries)
    for part in q_later:
        q_outer.append(outer_pairs(part, ranks))
    q_inner = inner_pairs(q_inner, ranks)

    sib_two = inner_pairs(two, ranks)
    sib_four = lax.ppermute(four, "dp", [(2 * m + 1, 2 * m) for m in pairs])
    window = (own, two, four, sib_own, sib_two, sib_four)

    direction = reward_dir.reshape(1, -1)
    attn_out, scores = None, []
    for i, heads in enumerate(SPLIT):
        last = i == len(SPLIT) - 1
        attn_out, score, *settled = attend(
            heads, info, place, q_own, q_outer[i], q_inner, window, direction, attn_out, scores,
            last, capacity, responses, ranks,
        )
        scores = [score]
    rewards = total_over(jnp.sum(settled[0], axis=1), ranks)
    return (attn_out, rewards)


def solution(mesh):
    return jax.shard_map(
        shards,
        mesh=mesh,
        in_specs=(
            P(("groups", "dp"), None),
            P(("groups", "dp"), None),
            P(("groups", "dp"), None),
            P(("groups", "dp")),
            P(("groups", "dp")),
            P(),
        ),
        out_specs=(P(("groups", "dp"), None), P("groups")),
        check_vma=False,
    )
```

```python
import functools
import math

import jax
import jax.numpy as jnp
from jax import lax
from jax.experimental import pallas as pl
from jax.experimental.pallas import tpu as pltpu
from jax.sharding import PartitionSpec as P

D_HEAD = 128
HEADS = 32
KV_HEADS = 4
BLOCK = 128
RECV = 2
REACH = 4
PER_GROUP = HEADS // KV_HEADS
ROWS = RECV * BLOCK
PIECES = REACH + 1
KV_WIDTH = KV_HEADS * D_HEAD
WIDTH = HEADS * D_HEAD
CHUNK = PER_GROUP * D_HEAD
STACKED = PER_GROUP * BLOCK
PAIR = 4
MASKED = -1e30
WIDE = pltpu.CompilerParams(vmem_limit_bytes=58 * 1024 * 1024 + 256 * 1024)
SLIM = pltpu.CompilerParams(vmem_limit_bytes=28 * 1024 * 1024)
EXP2_SCALE = D_HEAD ** (-0.5) * math.log2(math.e)
SPLIT = ((0,), (1, 2), (3,))

SMEM = pl.BlockSpec(memory_space=pltpu.SMEM)
VMEM = pl.BlockSpec(memory_space=pltpu.VMEM)
HBM = pl.BlockSpec(memory_space=pltpu.HBM)


def shifted(block, axis, distance):
    devices = range(lax.axis_size(axis))
    route = [(i - distance, i) for i in devices if i - distance in devices]
    return lax.ppermute(block, axis, route)


def inner_pairs(block, ranks):
    return lax.ppermute(block, "dp", [(i, i ^ 1) for i in range(ranks)])


def outer_pairs(block, ranks):
    route = []
    for low in range(1, ranks - 1, 2):
        route += [(low, low + 1), (low + 1, low)]
    return lax.ppermute(block, "dp", route)


def total_over(part, ranks):
    if ranks & (ranks - 1):
        return lax.psum(part, "dp")
    bit = 1
    while bit < ranks:
        steps = [bit, 2 * bit, 3 * bit] if 2 * bit < ranks else [bit]
        heard = [lax.ppermute(part, "dp", [(i, i ^ step) for i in range(ranks)]) for step in steps]
        part = part + sum(heard)
        bit *= 4
    return part


def block_rows(index):
    return pl.ds(pl.multiple_of(index * BLOCK, BLOCK), BLOCK)


def columns_of(heads):
    return pl.ds(heads[0] * CHUNK, len(heads) * CHUNK)


def transfer(copies):
    for copy in copies:
        copy.start()
    for copy in copies:
        copy.wait()


def end_rows(counts, place, capacity):
    tail = jnp.clip(counts[0] - RECV, 0, capacity - RECV) * BLOCK
    odd = lax.rem(place[0], 2) == 1
    outer = pl.multiple_of(jnp.where(odd, tail, 0), BLOCK)
    inner = pl.multiple_of(jnp.where(odd, 0, tail), BLOCK)
    return pl.ds(outer, ROWS), pl.ds(inner, ROWS)


def first_stage_kernel(capacity, counts, place, queries, keys, values, kv_outer, kv_inner, q_outer, sems):
    outer, inner = end_rows(counts, place, capacity)
    key_part, value_part = pl.ds(0, KV_WIDTH), pl.ds(KV_WIDTH, KV_WIDTH)
    transfer([
        pltpu.make_async_copy(keys.at[outer], kv_outer.at[:, key_part], sems.at[0]),
        pltpu.make_async_copy(values.at[outer], kv_outer.at[:, value_part], sems.at[1]),
        pltpu.make_async_copy(keys.at[inner], kv_inner.at[:, key_part], sems.at[2]),
        pltpu.make_async_copy(values.at[inner], kv_inner.at[:, value_part], sems.at[3]),
        pltpu.make_async_copy(queries.at[outer, columns_of(SPLIT[0])], q_outer, sems.at[4]),
    ])


def first_stage(counts, place, queries, keys, values):
    capacity = queries.shape[0] // BLOCK
    kv = jax.ShapeDtypeStruct((ROWS, 2 * KV_WIDTH), keys.dtype)
    q = jax.ShapeDtypeStruct((ROWS, len(SPLIT[0]) * CHUNK), queries.dtype)
    return pl.pallas_call(
        functools.partial(first_stage_kernel, capacity),
        out_shape=(kv, kv, q),
        in_specs=[SMEM, SMEM, HBM, HBM, HBM],
        out_specs=(VMEM, VMEM, VMEM),
        scratch_shapes=[pltpu.SemaphoreType.DMA((5,))],
        compiler_params=WIDE,
        name="first_stage",
    )(counts, place, queries, keys, values)


def second_stage_kernel(capacity, counts, place, queries, *rest):
    outs, sems = rest[:-1], rest[-1]
    outer, inner = end_rows(counts, place, capacity)
    copies = [
        pltpu.make_async_copy(queries.at[outer, columns_of(heads)], out, sems.at[i])
        for i, (heads, out) in enumerate(zip(SPLIT[1:], outs))
    ]
    copies.append(pltpu.make_async_copy(queries.at[inner], outs[-1], sems.at[len(SPLIT) - 1]))
    transfer(copies)


def second_stage(counts, place, queries):
    capacity = queries.shape[0] // BLOCK
    widths = [len(heads) * CHUNK for heads in SPLIT[1:]] + [WIDTH]
    return pl.pallas_call(
        functools.partial(second_stage_kernel, capacity),
        out_shape=tuple(jax.ShapeDtypeStruct((ROWS, width), queries.dtype) for width in widths),
        in_specs=[SMEM, SMEM, HBM],
        out_specs=(VMEM,) * len(widths),
        scratch_shapes=[pltpu.SemaphoreType.DMA((len(SPLIT),))],
        compiler_params=pltpu.CompilerParams(vmem_limit_bytes=48 * 1024 * 1024),
        name="second_stage",
    )(counts, place, queries)


def placement(info, place, responses, ranks):
    rank = place[0]
    before = lax.fori_loop(
        0, ranks, lambda s, t: t + jnp.where(s < rank, info[responses + s], 0), jnp.int32(0)
    )
    left_count = info[responses + jnp.maximum(rank - 1, 0)]
    return rank, before - rank * RECV, info[responses + rank], left_count


def pick(k, rank, excess, count, left_count, capacity):
    left_first = jnp.clip(left_count - RECV, 0, capacity - RECV)
    from_left = k < excess
    slot = k - excess
    is_own = jnp.logical_and(jnp.logical_not(from_left), slot < count)
    odd = lax.rem(rank, 2)
    left_kind, right_kind = jnp.where(odd == 1, 2, 0), jnp.where(odd == 1, 0, 2)
    kind = jnp.where(from_left, left_kind, jnp.where(is_own, 1, right_kind))
    index = jnp.where(
        from_left, left_count - excess + k - left_first, jnp.where(is_own, slot, slot - count)
    )
    limit = jnp.where(is_own, capacity - 1, RECV - 1)
    return kind, jnp.clip(index, 0, limit)


def pack_kernel(
    responses, ranks, capacity,
    info, place, queries, keys, values, outer, inner,
    out, q_own, sems,
):
    rank, excess, count, left_count = placement(info, place, responses, ranks)
    picks = [pick(k, rank, excess, count, left_count, capacity) for k in range(RECV)]
    jobs = []
    key_part, value_part = pl.ds(0, KV_WIDTH), pl.ds(KV_WIDTH, KV_WIDTH)
    for k, (kind, index) in enumerate(picks):
        rows = block_rows(index)
        into = pl.ds(k * BLOCK, BLOCK)
        mine = kind == 1
        jobs += [
            (mine, pltpu.make_async_copy(keys.at[rows], out.at[into, key_part], sems.at[k, 0])),
            (mine, pltpu.make_async_copy(values.at[rows], out.at[into, value_part], sems.at[k, 1])),
            (mine, pltpu.make_async_copy(queries.at[rows], q_own.at[into], sems.at[k, 2])),
        ]
    each(jobs, "start")

    for k, (kind, index) in enumerate(picks):
        for wanted, source in ((0, outer), (2, inner)):
            @pl.when(kind == wanted)
            def _(source=source, k=k, index=index):
                out[k * BLOCK:(k + 1) * BLOCK, :] = source[block_rows(index), :]
    each(jobs, "wait")


def pack(info, place, queries, keys, values, outer, inner, responses, ranks):
    capacity = keys.shape[0] // BLOCK
    return pl.pallas_call(
        functools.partial(pack_kernel, responses, ranks, capacity),
        out_shape=(
            jax.ShapeDtypeStruct((ROWS, 2 * KV_WIDTH), keys.dtype),
            jax.ShapeDtypeStruct((ROWS, WIDTH), queries.dtype),
        ),
        in_specs=[SMEM, SMEM, HBM, HBM, HBM, VMEM, VMEM],
        out_specs=(VMEM, VMEM),
        scratch_shapes=[
            pltpu.SemaphoreType.DMA((RECV, 3)),
        ],
        compiler_params=pltpu.CompilerParams(vmem_limit_bytes=48 * 1024 * 1024),
        name="pack",
    )(info, place, queries, keys, values, outer, inner)


def fill_window(rank, window, head, lowest, kbuf, vbuf):
    own, two, four, sib_own, sib_two, sib_four = window
    odd = lax.rem(rank, 2) == 1
    even = jnp.logical_not(odd)
    sources = ((None, own, 4), (odd, sib_own, 3), (even, sib_two, 3), (None, two, 2),
               (odd, sib_two, 1), (even, sib_four, 1), (None, four, 0))
    for condition, source, piece in sources:
        needed = lowest <= piece
        if condition is not None:
            needed = jnp.logical_and(needed, condition)

        @pl.when(needed)
        def _(source=source, piece=piece):
            kbuf[piece] = source[:, head * D_HEAD:(head + 1) * D_HEAD]
            vbuf[piece] = source[:, KV_WIDTH + head * D_HEAD:KV_WIDTH + (head + 1) * D_HEAD]


def each(jobs, action):
    for condition, copy in jobs:
        if condition is None:
            getattr(copy, action)()
        else:
            pl.when(condition)(getattr(copy, action))


def attend_kernel(
    responses, ranks, capacity, heads, earlier, rewards,
    info, place, q_own, q_outer, q_inner, own, two, four, sib_own, sib_two, sib_four,
    reward_dir, out, score, kbuf, vbuf, qbuf, obuf, sbuf, mbuf, lbuf, abuf, o_sems,
):
    rank, excess, count, left_count = placement(info, place, responses, ranks)
    columns = slice(heads[0] * CHUNK, (heads[-1] + 1) * CHUNK)
    for k in range(RECV):
        kind, index = pick(k, rank, excess, count, left_count, capacity)

        @pl.when(kind == 0)
        def _(k=k, index=index):
            qbuf[k] = q_outer[block_rows(index), :]

        @pl.when(kind == 1)
        def _(k=k):
            qbuf[k] = q_own[k * BLOCK:(k + 1) * BLOCK, columns]

        @pl.when(kind == 2)
        def _(k=k, index=index):
            qbuf[k] = q_inner[block_rows(index), columns]

    window = (own, two, four, sib_own, sib_two, sib_four)
    window_base = (rank - REACH) * ROWS
    first = rank * ROWS
    row_iota = lax.broadcasted_iota(jnp.int32, (ROWS, D_HEAD), 0)
    lane_iota = lax.broadcasted_iota(jnp.int32, (BLOCK, D_HEAD), 1)
    rows_at = row_iota + first

    def widen(r, carry):
        begin, begins = carry
        start = info[r]
        begin = jnp.where(start <= first, jnp.maximum(begin, start), begin)
        begins = jnp.where(rows_at >= start, jnp.maximum(begins, start), begins)
        return begin, begins

    begin, begins = lax.fori_loop(
        0, responses, widen, (jnp.int32(0), jnp.zeros((ROWS, D_HEAD), jnp.int32))
    )
    lowest = jnp.clip((begin - window_base) // ROWS, 0, REACH)

    stores = []
    score[...] = jnp.zeros_like(score)
    for at, head in enumerate(heads):
        fill_window(rank, window, head, lowest, kbuf, vbuf)
        mbuf[...] = jnp.full_like(mbuf, MASKED)

        def score_tile(p, _):
            base = window_base + p * ROWS
            key_tile = kbuf[p]
            for k in range(RECV):
                block = slice(k * BLOCK, (k + 1) * BLOCK)
                masks = []
                for half in range(2):
                    key_at = lane_iota + (base + half * D_HEAD)
                    masks.append(jnp.logical_and(key_at >= begins[block], key_at <= rows_at[block]))
                for j in range(0, PER_GROUP, PAIR):
                    parts = [
                        qbuf[k, :, at * CHUNK + i * D_HEAD:at * CHUNK + (i + 1) * D_HEAD]
                        for i in range(j, j + PAIR)
                    ]
                    logits = lax.dot_general(
                        jnp.concatenate(parts, axis=0), key_tile, (((1,), (1,)), ((), ())),
                        preferred_element_type=jnp.float32,
                    )
                    for i in range(PAIR):
                        rows = pl.ds(k * STACKED + (j + i) * BLOCK, BLOCK)
                        part = logits[i * BLOCK:(i + 1) * BLOCK]
                        low = jnp.where(masks[0], part[:, :D_HEAD], MASKED)
                        high = jnp.where(masks[1], part[:, D_HEAD:], MASKED)
                        sbuf[p, rows, :D_HEAD] = low
                        sbuf[p, rows, D_HEAD:] = high
                        mbuf[rows, :] = jnp.maximum(mbuf[rows, :], jnp.maximum(low, high))
            return 0

        lax.fori_loop(lowest, PIECES, score_tile, 0)
        for i in range(RECV * PER_GROUP):
            rows = pl.ds(i * BLOCK, BLOCK)
            peak = jnp.max(mbuf[rows, :], axis=-1, keepdims=True)
            mbuf[rows, :] = jnp.broadcast_to(peak, (BLOCK, D_HEAD))
        lbuf[...] = jnp.zeros_like(lbuf)
        abuf[...] = jnp.zeros_like(abuf)

        def weigh_tile(p, _):
            value_tile = vbuf[p]
            for i in range(0, RECV * PER_GROUP, PAIR):
                rows = pl.ds(i * BLOCK, PAIR * BLOCK)
                peak = mbuf[rows, :]
                low = jnp.exp2((sbuf[p, rows, :D_HEAD] - peak) * EXP2_SCALE)
                high = jnp.exp2((sbuf[p, rows, D_HEAD:] - peak) * EXP2_SCALE)
                lbuf[rows, :] += low + high
                soft = jnp.concatenate([low.astype(jnp.bfloat16), high.astype(jnp.bfloat16)], axis=1)
                abuf[rows, :] += jnp.dot(soft, value_tile, preferred_element_type=jnp.float32)
            return 0

        lax.fori_loop(lowest, PIECES, weigh_tile, 0)
        for k in range(RECV):
            scored = score[k * BLOCK:(k + 1) * BLOCK, :]
            for j in range(PER_GROUP):
                rows = pl.ds(k * STACKED + j * BLOCK, BLOCK)
                totals = jnp.sum(lbuf[rows, :], axis=-1, keepdims=True)
                into = slice(at * CHUNK + j * D_HEAD, at * CHUNK + (j + 1) * D_HEAD)
                head_out = (abuf[rows, :] / totals).astype(jnp.bfloat16)
                obuf[k, :, into] = head_out
                direction = reward_dir[:, head * CHUNK + j * D_HEAD:head * CHUNK + (j + 1) * D_HEAD]
                scored += head_out.astype(jnp.float32) * direction
            score[k * BLOCK:(k + 1) * BLOCK, :] = scored
            store = pltpu.make_async_copy(
                obuf.at[k, :, pl.ds(at * CHUNK, CHUNK)],
                out.at[pl.ds(k * BLOCK, BLOCK), pl.ds(head * CHUNK, CHUNK)],
                o_sems.at[at, k],
            )
            store.start()
            stores.append(store)
    if earlier:
        score[...] += sum(part[...] for part in earlier)
    if rewards is not None:
        def settle(r, _):
            following = info[jnp.minimum(r + 1, responses - 1)]
            at = jnp.where(r + 1 < responses, following, ranks * ROWS) - 1 - first
            here = jnp.logical_and(at >= 0, at < ROWS)
            row = score[pl.ds(jnp.clip(at, 0, ROWS - 1), 1), :]
            rewards[pl.ds(r, 1), :] = jnp.where(here, row, 0.0)
            return 0

        lax.fori_loop(0, responses, settle, 0)
    for store in stores:
        store.wait()


def attend(
    heads, info, place, q_own, q_outer, q_inner, window, reward_dir, previous, scores, last,
    capacity, responses, ranks,
):
    operands = [info, place, q_own, q_outer, q_inner, *window, reward_dir]
    used = len(operands)
    in_specs = [SMEM, SMEM] + [VMEM] * 10
    aliases = {}
    if previous is not None:
        aliases = {used: 0}
        operands += [previous] + scores
        in_specs += [HBM] + [VMEM] * len(scores)
    taken = len(operands)
    out_shape = [
        jax.ShapeDtypeStruct((ROWS, WIDTH), jnp.bfloat16),
        jax.ShapeDtypeStruct((ROWS, D_HEAD), jnp.float32),
    ]
    if last:
        out_shape.append(jax.ShapeDtypeStruct((responses, D_HEAD), jnp.float32))
    made = taken + len(out_shape)

    def body(*refs):
        attend_kernel(
            responses, ranks, capacity, heads, refs[used + 1:taken], refs[made - 1] if last else None,
            *refs[:used], *refs[taken:taken + 2], *refs[made:],
        )

    number = len(heads)
    return pl.pallas_call(
        body,
        out_shape=out_shape,
        in_specs=in_specs,
        out_specs=[HBM] + [VMEM] * (len(out_shape) - 1),
        scratch_shapes=[
            pltpu.VMEM((PIECES, ROWS, D_HEAD), jnp.bfloat16),
            pltpu.VMEM((PIECES, ROWS, D_HEAD), jnp.bfloat16),
            pltpu.VMEM((RECV, BLOCK, number * CHUNK), jnp.bfloat16),
            pltpu.VMEM((RECV, BLOCK, number * CHUNK), jnp.bfloat16),
            pltpu.VMEM((PIECES, RECV * STACKED, ROWS), jnp.float32),
            pltpu.VMEM((RECV * STACKED, D_HEAD), jnp.float32),
            pltpu.VMEM((RECV * STACKED, D_HEAD), jnp.float32),
            pltpu.VMEM((RECV * STACKED, D_HEAD), jnp.float32),
            pltpu.SemaphoreType.DMA((number, RECV)),
        ],
        input_output_aliases=aliases,
        compiler_params=SLIM,
        cost_estimate=pl.CostEstimate(
            flops=4 * number * RECV * STACKED * PIECES * ROWS * D_HEAD,
            bytes_accessed=2 * number * 1024 * 1024,
            transcendentals=number * RECV * STACKED * PIECES * ROWS,
        ),
    )(*operands)


def shards(queries, keys, values, block_counts, segment_ids, reward_dir):
    ranks = lax.axis_size("dp")
    rank = lax.axis_index("dp")
    capacity = queries.shape[0] // BLOCK
    responses = ranks * 2 // REACH
    place = rank.astype(jnp.int32).reshape(1)

    kv_outer, kv_inner, q_first = first_stage(block_counts, place, queries, keys, values)
    kv_outer = outer_pairs(kv_outer, ranks)
    kv_inner = inner_pairs(kv_inner, ranks)
    q_outer = [outer_pairs(q_first, ranks)]

    ids = jnp.arange(responses, dtype=jnp.int32)
    smaller = jnp.sum((segment_ids[None, :] < ids[:, None]).astype(jnp.int32), axis=1)
    marks = jnp.where(jnp.arange(ranks, dtype=jnp.int32) == rank, block_counts[0], 0)
    info = lax.psum(jnp.concatenate([smaller, marks]), "dp")

    own, q_own = pack(info, place, queries, keys, values, kv_outer, kv_inner, responses, ranks)
    two = shifted(own, "dp", 2)
    four = shifted(own, "dp", 4)
    pairs = range(ranks // 2)
    sib_own = lax.ppermute(own, "dp", [(2 * m, 2 * m + 1) for m in pairs])

    *q_later, q_inner = second_stage(block_counts, place, queries)
    for part in q_later:
        q_outer.append(outer_pairs(part, ranks))
    q_inner = inner_pairs(q_inner, ranks)

    sib_two = inner_pairs(two, ranks)
    sib_four = lax.ppermute(four, "dp", [(2 * m + 1, 2 * m) for m in pairs])
    window = (own, two, four, sib_own, sib_two, sib_four)

    direction = reward_dir.reshape(1, -1)
    attn_out, scores = None, []
    for i, heads in enumerate(SPLIT):
        last = i == len(SPLIT) - 1
        attn_out, score, *settled = attend(
            heads, info, place, q_own, q_outer[i], q_inner, window, direction, attn_out, scores,
            last, capacity, responses, ranks,
        )
        scores = [score]
    rewards = total_over(jnp.sum(settled[0], axis=1), ranks)
    return (attn_out, rewards)


def solution(mesh):
    return jax.shard_map(
        shards,
        mesh=mesh,
        in_specs=(
            P(("groups", "dp"), None),
            P(("groups", "dp"), None),
            P(("groups", "dp"), None),
            P(("groups", "dp")),
            P(("groups", "dp")),
            P(),
        ),
        out_specs=(P(("groups", "dp"), None), P("groups")),
        check_vma=False,
    )
```
